32 devices in a mesh: tm: 4 (over y, x), paths: 8 (over z, core).
Axes of the slice: x: 2, y: 2, z: 4, core: 2. Of those that a mesh axis runs over, the one named last changes fastest.
Arguments:
- returns: bfloat16 [128, 4096, 256], P('tm', 'paths'), may hold values from -0.15917969 to 0.15917969
- weights: bfloat16 [256, 64], P('paths'), may hold values from -0.375 to 0.375
Outputs:
- drawdown: float32 [64, 4096], P('tm', 'paths')
The draws below stay inside these ranges and needn't reach their ends.
All inputs are finite; a program needn't handle non-finite values.
Results may differ from the reference program's by a relative error of at most 0.0003.
Values may be sent and summed in bfloat16 or wider, within the bound.
No kernel may reach another device: no remote copies, remote signals or barrier semaphores. Data moves between devices by JAX's collectives and lax.ppermute only.
A program may use at most 64 MiB of HBM per device.

```python
import jax
import jax.numpy as jnp
from jax import lax

ASSETS = 256
PORT = 64
T_DEV = 32
STEPS = 128
PATHS = 4096
N_TM = 4


def block_levels(key, shape, shards, smallest, high):
    loudness = 1.0
    for dim, parts in shards:
        heights = jax.random.uniform(jax.random.fold_in(jax.random.fold_in(key, 6), dim), (parts,), jnp.float32, smallest / len(shards), high / len(shards))
        loudness = loudness * jnp.repeat(jnp.exp(heights), shape[dim] // parts).reshape((-1,) + (1,) * (len(shape) - 1 - dim))
    return loudness


def bell_draw(stream_key, dims, spread, limit, split=(), kind=jnp.bfloat16):
    loudness = block_levels(stream_key, dims, split, -0.22, 0.18) if split else 1.0
    array = jax.random.normal(stream_key, dims, jnp.float32) * spread * loudness
    return jnp.minimum(jnp.maximum(array, -limit), limit).astype(kind)


def setup_inputs(seed: int = 0) -> dict:
    keys = jax.random.split(jax.random.key(seed), 3)
    return {
        "returns": bell_draw(keys[0], (STEPS, PATHS, ASSETS), 0.02, 0.15917969, ((0, 4), (1, 8))),
        "weights": bell_draw(keys[1], (ASSETS, PORT), ASSETS ** -0.5, 0.375, ((0, 8),)),
    }


def reference(returns, weights):
    blocks = returns.reshape(N_TM, T_DEV, PATHS, ASSETS)
    holdings = weights.astype(jnp.float32)

    def advance(carry, block):
        level, highest, deepest = carry
        profit = jnp.einsum('tpa,aq->tqp', block.astype(jnp.float32), holdings)
        value = level[None] + jnp.cumsum(profit, axis=0)
        running = jnp.maximum(highest[None], lax.cummax(value, axis=0))
        deepest = jnp.maximum(deepest, jnp.max(running - value, axis=0))
        return (value[-1], running[-1], deepest), None

    zeros = jnp.zeros((PORT, PATHS), jnp.float32)
    final, unused = lax.scan(advance, (zeros, zeros, zeros), blocks)
    return final[2]
```

```python
import functools

import jax
import jax.numpy as jnp
from jax import lax
from jax.experimental import pallas as pl
from jax.experimental.pallas import tpu as pltpu
from jax.sharding import PartitionSpec as P


def gather_weights(weights):
    count = lax.axis_size("paths")
    place = lax.axis_index("paths")
    rows = weights
    step = 1
    while step < count:
        other = lax.ppermute(rows, "paths", [(s, s ^ step) for s in range(count)])
        low = (place & step) == 0
        rows = jnp.where(low, jnp.concatenate([rows, other]), jnp.concatenate([other, rows]))
        step *= 2
    return rows


def segment_kernel(segments, tile, weights_ref, returns_ref, *refs):
    outs = refs[:segments]
    block, arrived, stats = refs[segments:]
    steps, paths, assets = returns_ref.shape
    ports = weights_ref.shape[1]
    width = ports // segments

    def fetch(t):
        return pltpu.make_async_copy(returns_ref.at[t], block.at[t], arrived.at[t])

    for t in range(steps):
        fetch(t).start()

    own = lax.axis_index("tm")
    row = lax.broadcasted_iota(jnp.int32, (ports, ports), 0)
    col = lax.broadcasted_iota(jnp.int32, (ports, ports), 1)
    pick = col == ((row // width) ^ own) * width + row % width
    contract_last = (((1,), (1,)), ((), ()))
    turned = lax.dot_general(
        pick.astype(jnp.bfloat16), weights_ref[...], contract_last,
        preferred_element_type=jnp.float32,
    ).astype(jnp.bfloat16)

    stats[...] = jnp.zeros_like(stats)
    lanes = min(256, paths)

    def group(g, carry):
        first = g * tile
        for i in range(tile):
            fetch(first + i).wait()
        for c in range(0, paths, lanes):
            profits = [
                lax.dot_general(
                    turned, block[first + i, c : c + lanes, :], contract_last,
                    preferred_element_type=jnp.float32,
                )
                for i in range(tile)
            ]
            for q in range(0, ports, 16):
                at = (pl.ds(q, 16), pl.ds(c, lanes))
                value, peak, low, fall = (stats[(n, *at)] for n in range(4))
                for i in range(tile):
                    value = value + profits[i][q : q + 16]
                    peak = jnp.maximum(peak, value)
                    low = jnp.minimum(low, value)
                    fall = jnp.maximum(fall, peak - value)
                for n, new in enumerate((value, peak, low, fall)):
                    stats[(n, *at)] = new
        return carry

    lax.fori_loop(0, steps // tile, group, 0)

    for k in range(segments):
        at = slice(k * width, (k + 1) * width)
        outs[k][0] = stats[3, at]
        outs[k][1] = stats[2, at]
        outs[k][2] = stats[1, at] - stats[0, at]
        outs[k][3] = stats[0, at]


def join_kernel(segments, *refs):
    ins, out_ref, ordered = refs[:segments], refs[segments], refs[segments + 1]
    own = lax.axis_index("tm")
    for k in range(segments):
        ordered[own ^ k] = ins[k][...]
    fall = ordered[0, 0]
    drop = ordered[0, 2]
    for s in range(1, segments):
        fall = jnp.maximum(jnp.maximum(fall, ordered[s, 0]), drop - ordered[s, 1])
        drop = jnp.maximum(drop - ordered[s, 3], ordered[s, 2])
    out_ref[...] = fall


def shards(returns, weights):
    segments = lax.axis_size("tm")
    steps, paths, assets = returns.shape
    ports = weights.shape[1]
    width = ports // segments
    tile = 8 if steps % 8 == 0 else 1
    part = jax.ShapeDtypeStruct((4, width, paths), jnp.float32)
    vmem = pl.BlockSpec(memory_space=pltpu.VMEM)
    all_weights = gather_weights(weights)
    parts = pl.pallas_call(
        functools.partial(segment_kernel, segments, tile),
        out_shape=[part] * segments,
        in_specs=[vmem, pl.BlockSpec(memory_space=pltpu.HBM)],
        out_specs=[vmem] * segments,
        scratch_shapes=[
            pltpu.VMEM((steps, paths, assets), returns.dtype),
            pltpu.SemaphoreType.DMA((steps,)),
            pltpu.VMEM((4, ports, paths), jnp.float32),
        ],
        compiler_params=pltpu.CompilerParams(vmem_limit_bytes=24 * 2**20),
        name="segment",
    )(all_weights, returns)
    arrived = [parts[0]] + [
        lax.ppermute(parts[k], "tm", [(s, s ^ k) for s in range(segments)])
        for k in range(1, segments)
    ]
    return pl.pallas_call(
        functools.partial(join_kernel, segments),
        out_shape=jax.ShapeDtypeStruct((width, paths), jnp.float32),
        in_specs=[vmem] * segments,
        out_specs=vmem,
        scratch_shapes=[pltpu.VMEM((segments, 4, width, paths), jnp.float32)],
        compiler_params=pltpu.CompilerParams(vmem_limit_bytes=8 * 2**20),
        name="join",
    )(*arrived)


def solution(mesh):
    in_specs = (P("tm", "paths", None), P("paths", None))
    out_specs = P("tm", "paths")
    return jax.shard_map(shards, mesh=mesh, in_specs=in_specs, out_specs=out_specs, check_vma=False)
```

```python
import functools

import jax
import jax.numpy as jnp
from jax import lax
from jax.experimental import pallas as pl
from jax.experimental.pallas import tpu as pltpu
from jax.sharding import PartitionSpec as P

CONTRACT_LAST = (((1,), (1,)), ((), ()))
VMEM = pl.BlockSpec(memory_space=pltpu.VMEM)
HBM = pl.BlockSpec(memory_space=pltpu.HBM)


def dot_last(a, b):
    return lax.dot_general(a, b, CONTRACT_LAST, preferred_element_type=jnp.float32)


def call(kernel, name, out_shape, args, scratch=(), kept=(), limit=8, flops=0, moved=0):
    args = [
        pltpu.with_memory_space_constraint(a, pltpu.HBM) if i in kept else a
        for i, a in enumerate(args)
    ]
    several = isinstance(out_shape, (list, tuple))
    return pl.pallas_call(
        kernel,
        out_shape=out_shape,
        in_specs=[HBM if i in kept else VMEM for i in range(len(args))],
        out_specs=[VMEM] * len(out_shape) if several else VMEM,
        scratch_shapes=list(scratch),
        compiler_params=pltpu.CompilerParams(vmem_limit_bytes=limit * 2**20),
        cost_estimate=pl.CostEstimate(flops=flops, bytes_accessed=moved, transcendentals=0),
        name=name,
    )(*args)


def swap(rows, bit):
    count = lax.axis_size("paths")
    return lax.ppermute(rows, "paths", [(s, s ^ bit) for s in range(count)])


def stage_kernel(weights_ref, returns_ref, out_ref):
    out_ref[...] = weights_ref[...]


def merge_kernel(bit, rows_ref, other_ref, out_ref):
    count = rows_ref.shape[0]
    upper = (lax.axis_index("paths") // bit) % 2
    out_ref[pl.ds(pl.multiple_of(upper * count, count), count)] = rows_ref[...]
    out_ref[pl.ds(pl.multiple_of((1 - upper) * count, count), count)] = other_ref[...]


def spread(segments, rows):
    assets, ports = rows.shape
    width = ports // segments
    own = lax.axis_index("tm")
    row = lax.broadcasted_iota(jnp.int32, (ports, ports), 0)
    col = lax.broadcasted_iota(jnp.int32, (ports, ports), 1)
    pick = (col == ((row // width) ^ own) * width + row % width).astype(jnp.bfloat16)
    turned = dot_last(pick, rows).astype(jnp.bfloat16)
    blank = jnp.zeros_like(turned)
    return jnp.concatenate(
        [jnp.concatenate([turned, blank], axis=1), jnp.concatenate([blank, turned], axis=1)]
    )


def half_profit(spread_rows, returns_ref, t, half):
    paths, assets = returns_ref.shape[1:]
    columns = pl.ds(pl.multiple_of(half * (assets // 2), assets // 2), assets // 2)
    both = jnp.concatenate(
        [returns_ref[t, : paths // 2, columns], returns_ref[t, paths // 2 :, columns]], axis=1
    )
    return dot_last(spread_rows, both)


def first_kernel(segments, rows_ref, returns_ref, out_ref):
    half = lax.axis_index("paths") // (lax.axis_size("paths") // 2)
    rows = spread(segments, rows_ref[...])
    for t in range(returns_ref.shape[0]):
        out_ref[t] = half_profit(rows, returns_ref, t, half)


def second_kernel(segments, tile, rows_ref, returns_ref, first_ref, *refs):
    outs, stats = refs[:segments], refs[segments]
    steps, paths, assets = returns_ref.shape
    ports = rows_ref.shape[1]
    width = ports // segments
    half = 1 - lax.axis_index("paths") // (lax.axis_size("paths") // 2)
    rows = spread(segments, rows_ref[...])
    stats[...] = jnp.zeros_like(stats)
    for g in range(0, steps, tile):
        profits = [half_profit(rows, returns_ref, g + i, half) for i in range(tile)]
        for q in range(0, 2 * ports, 16):
            value, peak, low, fall = (stats[n, q : q + 16] for n in range(4))
            for i in range(tile):
                value = value + (first_ref[g + i, q : q + 16] + profits[i][q : q + 16])
                peak = jnp.maximum(peak, value)
                low = jnp.minimum(low, value)
                fall = jnp.maximum(fall, peak - value)
            for n, new in enumerate((value, peak, low, fall)):
                stats[n, q : q + 16] = new
    for k in range(segments):
        for h in range(2):
            at = slice(h * ports + k * width, h * ports + (k + 1) * width)
            put = slice(h * (paths // 2), (h + 1) * (paths // 2))
            outs[k][0, :, put] = stats[3, at]
            outs[k][1, :, put] = stats[2, at]
            outs[k][2, :, put] = stats[1, at] - stats[0, at]
            outs[k][3, :, put] = stats[0, at]


def join_kernel(segments, *refs):
    ins, out_ref, ordered = refs[:segments], refs[segments], refs[segments + 1]
    own = lax.axis_index("tm")
    for k in range(segments):
        ordered[own ^ k] = ins[k][...]
    fall = ordered[0, 0]
    drop = ordered[0, 2]
    for s in range(1, segments):
        fall = jnp.maximum(jnp.maximum(fall, ordered[s, 0]), drop - ordered[s, 1])
        drop = jnp.maximum(drop - ordered[s, 3], ordered[s, 2])
    out_ref[...] = fall


def shards(returns, weights):
    segments = lax.axis_size("tm")
    count = lax.axis_size("paths")
    steps, paths, assets = returns.shape
    ports = weights.shape[1]
    width = ports // segments
    held = jax.ShapeDtypeStruct((steps, 2 * ports, paths // 2), jnp.float32)
    part = jax.ShapeDtypeStruct((4, width, paths), jnp.float32)
    work = 2 * steps * paths * assets * ports

    rows = call(
        stage_kernel, "stage", jax.ShapeDtypeStruct(weights.shape, weights.dtype), [weights, returns],
        kept=(1,), flops=work, moved=returns.size * 2,
    )
    other = swap(weights, 1)
    bit = 1
    while 2 * bit < count:
        rows = call(
            functools.partial(merge_kernel, bit), f"merge{bit}",
            jax.ShapeDtypeStruct((2 * rows.shape[0], ports), rows.dtype), [rows, other],
        )
        bit *= 2
        other = swap(rows, bit)
    first = call(
        functools.partial(first_kernel, segments), "first", held, [rows, returns],
        flops=work, moved=returns.size,
    )
    parts = call(
        functools.partial(second_kernel, segments, min(steps, 8)), "second", [part] * segments,
        [other, returns, first],
        scratch=[pltpu.VMEM((4, 2 * ports, paths // 2), jnp.float32)],
        flops=work, moved=returns.size,
    )
    arrived = [parts[0]] + [
        lax.ppermute(parts[k], "tm", [(s, s ^ k) for s in range(segments)])
        for k in range(1, segments)
    ]
    return call(
        functools.partial(join_kernel, segments), "join",
        jax.ShapeDtypeStruct((width, paths), jnp.float32), arrived,
        scratch=[pltpu.VMEM((segments, 4, width, paths), jnp.float32)],
        moved=8 * part.size,
    )


def solution(mesh):
    in_specs = (P("tm", "paths", None), P("paths", None))
    out_specs = P("tm", "paths")
    return jax.shard_map(shards, mesh=mesh, in_specs=in_specs, out_specs=out_specs, check_vma=False)
```

```python
import functools
import math

import jax
import jax.numpy as jnp
from jax import lax
from jax.experimental import pallas as pl
from jax.experimental.pallas import tpu as pltpu
from jax.sharding import PartitionSpec as P

CONTRACT_LAST = (((1,), (1,)), ((), ()))
MAX_RETURN = 0.15917969
MAX_WEIGHT = 0.375
VMEM = pl.BlockSpec(memory_space=pltpu.VMEM)
HBM = pl.BlockSpec(memory_space=pltpu.HBM)


def dot_last(a, b):
    return lax.dot_general(a, b, CONTRACT_LAST, preferred_element_type=jnp.float32)


def call(kernel, name, out_shape, args, scratch=(), kept=(), limit=8, flops=0, moved=0):
    args = [
        pltpu.with_memory_space_constraint(a, pltpu.HBM) if i in kept else a
        for i, a in enumerate(args)
    ]
    several = isinstance(out_shape, (list, tuple))
    return pl.pallas_call(
        kernel,
        out_shape=out_shape,
        in_specs=[HBM if i in kept else VMEM for i in range(len(args))],
        out_specs=[VMEM] * len(out_shape) if several else VMEM,
        scratch_shapes=list(scratch),
        compiler_params=pltpu.CompilerParams(vmem_limit_bytes=limit * 2**20),
        cost_estimate=pl.CostEstimate(flops=flops, bytes_accessed=moved, transcendentals=0),
        name=name,
    )(*args)


def swap(rows, bit):
    count = lax.axis_size("paths")
    return lax.ppermute(rows, "paths", [(s, s ^ bit) for s in range(count)])


def stage_kernel(weights_ref, returns_ref, out_ref):
    out_ref[...] = weights_ref[...]


def merge_kernel(bit, rows_ref, other_ref, out_ref):
    count = rows_ref.shape[0]
    upper = (lax.axis_index("paths") // bit) % 2
    out_ref[pl.ds(pl.multiple_of(upper * count, count), count)] = rows_ref[...]
    out_ref[pl.ds(pl.multiple_of((1 - upper) * count, count), count)] = other_ref[...]


def spread(segments, rows):
    assets, ports = rows.shape
    width = ports // segments
    own = lax.axis_index("tm")
    row = lax.broadcasted_iota(jnp.int32, (ports, ports), 0)
    col = lax.broadcasted_iota(jnp.int32, (ports, ports), 1)
    pick = (col == ((row // width) ^ own) * width + row % width).astype(jnp.bfloat16)
    turned = dot_last(pick, rows).astype(jnp.bfloat16)
    blank = jnp.zeros_like(turned)
    return jnp.concatenate(
        [jnp.concatenate([turned, blank], axis=1), jnp.concatenate([blank, turned], axis=1)]
    )


def half_profit(spread_rows, returns_ref, t, half):
    paths, assets = returns_ref.shape[1:]
    columns = pl.ds(pl.multiple_of(half * (assets // 2), assets // 2), assets // 2)
    both = jnp.concatenate(
        [returns_ref[t, : paths // 2, columns], returns_ref[t, paths // 2 :, columns]], axis=1
    )
    return dot_last(spread_rows, both)


def first_kernel(segments, rows_ref, returns_ref, out_ref):
    half = lax.axis_index("paths") // (lax.axis_size("paths") // 2)
    rows = spread(segments, rows_ref[...])
    for t in range(returns_ref.shape[0]):
        out_ref[t] = half_profit(rows, returns_ref, t, half)


def scale_of(terms):
    return 2.0 ** math.floor(math.log2(65504 / (terms * MAX_RETURN * MAX_WEIGHT)))


def encode(part, terms):
    part = part * scale_of(terms)
    wide = part * 8193.0
    near = wide - (wide - part)
    return jnp.where(part < near, -near, near)


def decode(sent, terms):
    sent = sent.astype(jnp.float32)
    return (jnp.abs(sent) + (0.75 * 2.0**-12) * sent) * (1 / scale_of(terms))


def second_kernel(segments, tile, rows_ref, returns_ref, first_ref, *refs):
    outs, stats = refs[:segments], refs[segments]
    steps, paths, assets = returns_ref.shape
    ports = rows_ref.shape[1]
    width = ports // segments
    half = 1 - lax.axis_index("paths") // (lax.axis_size("paths") // 2)
    rows = spread(segments, rows_ref[...])
    stats[...] = jnp.zeros_like(stats)
    for g in range(0, steps, tile):
        profits = [half_profit(rows, returns_ref, g + i, half) for i in range(tile)]
        for q in range(0, 2 * ports, 16):
            value, peak, low, fall = (stats[n, q : q + 16] for n in range(4))
            for i in range(tile):
                value = value + (first_ref[g + i, q : q + 16] + profits[i][q : q + 16])
                peak = jnp.maximum(peak, value)
                low = jnp.minimum(low, value)
                fall = jnp.maximum(fall, peak - value)
            for n, new in enumerate((value, peak, low, fall)):
                stats[n, q : q + 16] = new
    for k in range(segments):
        for h in range(2):
            at = slice(h * ports + k * width, h * ports + (k + 1) * width)
            put = slice(h * (paths // 2), (h + 1) * (paths // 2))
            value, peak, low, fall = (stats[n, at] for n in range(4))
            for n, part in enumerate((fall, -low, peak - value, value - low)):
                outs[k][n, :, put] = part if k == 0 else encode(part, steps * assets)


def join_kernel(segments, terms, *refs):
    ins, out_ref, ordered = refs[:segments], refs[segments], refs[segments + 1]
    own = lax.axis_index("tm")
    for k in range(segments):
        ordered[own ^ k] = ins[k][...] if k == 0 else decode(ins[k][...], terms)
    fall = ordered[0, 0]
    drop = ordered[0, 2]
    for s in range(1, segments):
        below = ordered[s, 1]
        fall = jnp.maximum(jnp.maximum(fall, ordered[s, 0]), drop + below)
        drop = jnp.maximum(drop + below - ordered[s, 3], ordered[s, 2])
    out_ref[...] = fall


def shards(returns, weights):
    segments = lax.axis_size("tm")
    count = lax.axis_size("paths")
    steps, paths, assets = returns.shape
    ports = weights.shape[1]
    width = ports // segments
    held = jax.ShapeDtypeStruct((steps, 2 * ports, paths // 2), jnp.float32)
    part = jax.ShapeDtypeStruct((4, width, paths), jnp.float32)
    work = 2 * steps * paths * assets * ports

    rows = call(
        stage_kernel, "stage", jax.ShapeDtypeStruct(weights.shape, weights.dtype), [weights, returns],
        kept=(1,), flops=work, moved=returns.size * 2,
    )
    other = swap(weights, 1)
    bit = 1
    while 2 * bit < count:
        rows = call(
            functools.partial(merge_kernel, bit), f"merge{bit}",
            jax.ShapeDtypeStruct((2 * rows.shape[0], ports), rows.dtype), [rows, other],
        )
        bit *= 2
        other = swap(rows, bit)
    first = call(
        functools.partial(first_kernel, segments), "first", held, [rows, returns],
        flops=work, moved=returns.size,
    )
    parts = call(
        functools.partial(second_kernel, segments, min(steps, 8)), "second", [part] * segments,
        [other, returns, first],
        scratch=[pltpu.VMEM((4, 2 * ports, paths // 2), jnp.float32)],
        flops=work, moved=returns.size,
    )
    arrived = [parts[0]] + [
        lax.ppermute(
            parts[k].astype(jnp.float16), "tm", [(s, s ^ k) for s in range(segments)]
        ).astype(jnp.float32)
        for k in range(1, segments)
    ]
    return call(
        functools.partial(join_kernel, segments, steps * assets), "join",
        jax.ShapeDtypeStruct((width, paths), jnp.float32), arrived,
        scratch=[pltpu.VMEM((segments, 4, width, paths), jnp.float32)],
        moved=8 * part.size,
    )


def solution(mesh):
    in_specs = (P("tm", "paths", None), P("paths", None))
    out_specs = P("tm", "paths")
    return jax.shard_map(shards, mesh=mesh, in_specs=in_specs, out_specs=out_specs, check_vma=False)
```

```python
import functools
import math

import jax
import jax.numpy as jnp
from jax import lax
from jax.experimental import pallas as pl
from jax.experimental.pallas import tpu as pltpu
from jax.sharding import PartitionSpec as P

CONTRACT_LAST = (((1,), (1,)), ((), ()))
SMALLEST = 2.0**-14
FINER = 2.0**28
MAX_RETURN = 0.15917969
MAX_WEIGHT = 0.375
VMEM = pl.BlockSpec(memory_space=pltpu.VMEM)
HBM = pl.BlockSpec(memory_space=pltpu.HBM)


def dot_last(a, b):
    return lax.dot_general(a, b, CONTRACT_LAST, preferred_element_type=jnp.float32)


def call(kernel, name, out_shape, args, scratch=(), kept=(), limit=8, flops=0, moved=0):
    args = [
        pltpu.with_memory_space_constraint(a, pltpu.HBM) if i in kept else a
        for i, a in enumerate(args)
    ]
    several = isinstance(out_shape, (list, tuple))
    return pl.pallas_call(
        kernel,
        out_shape=out_shape,
        in_specs=[HBM if i in kept else VMEM for i in range(len(args))],
        out_specs=[VMEM] * len(out_shape) if several else VMEM,
        scratch_shapes=list(scratch),
        compiler_params=pltpu.CompilerParams(vmem_limit_bytes=limit * 2**20),
        cost_estimate=pl.CostEstimate(flops=flops, bytes_accessed=moved, transcendentals=0),
        name=name,
    )(*args)


def swap(rows, bit):
    count = lax.axis_size("paths")
    return lax.ppermute(rows, "paths", [(s, s ^ (bit | 1)) for s in range(count)])


def stage_kernel(weights_ref, returns_ref, out_ref):
    out_ref[...] = weights_ref[...]


def merge_kernel(bit, rows_ref, other_ref, out_ref):
    count = rows_ref.shape[0]
    upper = (lax.axis_index("paths") // bit) % 2
    out_ref[pl.ds(pl.multiple_of(upper * count, count), count)] = rows_ref[...]
    out_ref[pl.ds(pl.multiple_of((1 - upper) * count, count), count)] = other_ref[...]


def spread(segments, rows):
    assets, ports = rows.shape
    width = ports // segments
    own = lax.axis_index("tm")
    row = lax.broadcasted_iota(jnp.int32, (ports, ports), 0)
    col = lax.broadcasted_iota(jnp.int32, (ports, ports), 1)
    pick = (col == ((row // width) ^ own) * width + row % width).astype(jnp.bfloat16)
    turned = dot_last(pick, rows).astype(jnp.bfloat16)
    blank = jnp.zeros_like(turned)
    return jnp.concatenate(
        [jnp.concatenate([turned, blank], axis=1), jnp.concatenate([blank, turned], axis=1)]
    )


def half_profit(spread_rows, returns_ref, t, half):
    paths, assets = returns_ref.shape[1:]
    columns = pl.ds(pl.multiple_of(half * (assets // 2), assets // 2), assets // 2)
    both = jnp.concatenate(
        [returns_ref[t, : paths // 2, columns], returns_ref[t, paths // 2 :, columns]], axis=1
    )
    return dot_last(spread_rows, both)


def first_kernel(segments, rows_ref, returns_ref, out_ref):
    half = lax.axis_index("paths") // (lax.axis_size("paths") // 2)
    rows = spread(segments, rows_ref[...])
    for t in range(returns_ref.shape[0]):
        out_ref[t] = half_profit(rows, returns_ref, t, half)


def scale_of(terms):
    return 2.0 ** math.floor(math.log2(65504 / (terms * MAX_RETURN * MAX_WEIGHT)))


def encode(part, terms):
    part = part * scale_of(terms)
    return jnp.where(part < SMALLEST, part * -FINER, part)


def decode(sent, terms):
    return jnp.where(sent < 0, sent * (-1 / (FINER * scale_of(terms))), sent * (1 / scale_of(terms)))


def second_kernel(segments, tile, rows_ref, returns_ref, first_ref, *refs):
    outs, stats = refs[:segments], refs[segments]
    steps, paths, assets = returns_ref.shape
    ports = rows_ref.shape[1]
    width = ports // segments
    half = 1 - lax.axis_index("paths") // (lax.axis_size("paths") // 2)
    rows = spread(segments, rows_ref[...])
    stats[...] = jnp.zeros_like(stats)
    for g in range(0, steps, tile):
        profits = [half_profit(rows, returns_ref, g + i, half) for i in range(tile)]
        for q in range(0, 2 * ports, 16):
            value, peak, low, fall = (stats[n, q : q + 16] for n in range(4))
            for i in range(tile):
                value = value + (first_ref[g + i, q : q + 16] + profits[i][q : q + 16])
                peak = jnp.maximum(peak, value)
                low = jnp.minimum(low, value)
                fall = jnp.maximum(fall, peak - value)
            for n, new in enumerate((value, peak, low, fall)):
                stats[n, q : q + 16] = new
    for k in range(segments):
        for h in range(2):
            at = slice(h * ports + k * width, h * ports + (k + 1) * width)
            put = slice(h * (paths // 2), (h + 1) * (paths // 2))
            value, peak, low, fall = (stats[n, at] for n in range(4))
            for n, part in enumerate((fall, -low, peak - value, value - low)):
                outs[k][n, :, put] = part if k == 0 else encode(part, steps * assets)


def join_kernel(segments, terms, *refs):
    ins, out_ref, ordered = refs[:segments], refs[segments], refs[segments + 1]
    own = lax.axis_index("tm")
    for k in range(segments):
        ordered[own ^ k] = ins[k][...] if k == 0 else decode(ins[k][...], terms)
    fall = ordered[0, 0]
    drop = ordered[0, 2]
    for s in range(1, segments):
        below = ordered[s, 1]
        fall = jnp.maximum(jnp.maximum(fall, ordered[s, 0]), drop + below)
        drop = jnp.maximum(drop + below - ordered[s, 3], ordered[s, 2])
    out_ref[...] = fall


def shards(returns, weights):
    segments = lax.axis_size("tm")
    count = lax.axis_size("paths")
    steps, paths, assets = returns.shape
    ports = weights.shape[1]
    width = ports // segments
    held = jax.ShapeDtypeStruct((steps, 2 * ports, paths // 2), jnp.float32)
    part = jax.ShapeDtypeStruct((4, width, paths), jnp.float32)
    work = 2 * steps * paths * assets * ports

    rows = call(
        stage_kernel, "stage", jax.ShapeDtypeStruct(weights.shape, weights.dtype), [weights, returns],
        kept=(1,), flops=work, moved=returns.size * 2,
    )
    other = swap(weights, 1)
    bit = 1
    while 2 * bit < count:
        rows = call(
            functools.partial(merge_kernel, bit), f"merge{bit}",
            jax.ShapeDtypeStruct((2 * rows.shape[0], ports), rows.dtype), [rows, other],
        )
        bit *= 2
        other = swap(rows, bit)
    first = call(
        functools.partial(first_kernel, segments), "first", held, [rows, returns],
        flops=work, moved=returns.size,
    )
    parts = call(
        functools.partial(second_kernel, segments, min(steps, 8)), "second", [part] * segments,
        [other, returns, first],
        scratch=[pltpu.VMEM((4, 2 * ports, paths // 2), jnp.float32)],
        flops=work, moved=returns.size,
    )
    arrived = [parts[0]] + [
        lax.ppermute(
            parts[k].astype(jnp.float16), "tm", [(s, s ^ k) for s in range(segments)]
        ).astype(jnp.float32)
        for k in range(1, segments)
    ]
    return call(
        functools.partial(join_kernel, segments, steps * assets), "join",
        jax.ShapeDtypeStruct((width, paths), jnp.float32), arrived,
        scratch=[pltpu.VMEM((segments, 4, width, paths), jnp.float32)],
        moved=8 * part.size,
    )


def solution(mesh):
    in_specs = (P("tm", "paths", None), P("paths", None))
    out_specs = P("tm", "paths")
    return jax.shard_map(shards, mesh=mesh, in_specs=in_specs, out_specs=out_specs, check_vma=False)
```

```python
import functools
import math

import jax
import jax.numpy as jnp
from jax import lax
from jax.experimental import pallas as pl
from jax.experimental.pallas import tpu as pltpu
from jax.sharding import PartitionSpec as P

SMALLEST = 2.0**-14
FINER = 2.0**28
MAX_RETURN = 0.15917969
MAX_WEIGHT = 0.375
VMEM = pl.BlockSpec(memory_space=pltpu.VMEM)
HBM = pl.BlockSpec(memory_space=pltpu.HBM)


def call(kernel, name, out_shape, args, scratch=(), kept=(), limit=8, flops=0, moved=0):
    args = [
        pltpu.with_memory_space_constraint(a, pltpu.HBM) if i in kept else a
        for i, a in enumerate(args)
    ]
    several = isinstance(out_shape, (list, tuple))
    return pl.pallas_call(
        kernel,
        out_shape=out_shape,
        in_specs=[HBM if i in kept else VMEM for i in range(len(args))],
        out_specs=[VMEM] * len(out_shape) if several else VMEM,
        scratch_shapes=list(scratch),
        compiler_params=pltpu.CompilerParams(vmem_limit_bytes=limit * 2**20),
        cost_estimate=pl.CostEstimate(flops=flops, bytes_accessed=moved, transcendentals=0),
        name=name,
    )(*args)


def swap(rows, bit):
    count = lax.axis_size("paths")
    return lax.ppermute(rows, "paths", [(s, s ^ (bit | 1)) for s in range(count)])


def stage_kernel(weights_ref, returns_ref, out_ref):
    out_ref[...] = weights_ref[...]


def pair_kernel(rows_ref, other_ref, out_ref):
    ports = rows_ref.shape[1]
    first = lax.axis_index("paths") % 2 == 0
    mine, other = rows_ref[...], other_ref[...]
    out_ref[:, :ports] = jnp.where(first, mine, other)
    out_ref[:, ports:] = jnp.where(first, other, mine)


def merge_kernel(bit, rows_ref, other_ref, out_ref):
    count = rows_ref.shape[0]
    upper = (lax.axis_index("paths") // bit) % 2
    out_ref[pl.ds(pl.multiple_of(upper * count, count), count)] = rows_ref[...]
    out_ref[pl.ds(pl.multiple_of((1 - upper) * count, count), count)] = other_ref[...]


def lay_out(shard, rows_ref, both_ref):
    ports = rows_ref.shape[1] // 2
    assets = both_ref.shape[0] // 2
    both_ref[...] = jnp.zeros_like(both_ref)
    for h in range(2):
        for n in range(assets // shard):
            block = slice(n // 2 * shard, (n // 2 + 1) * shard)
            core = slice(n % 2 * ports, (n % 2 + 1) * ports)
            at = h * assets + n * shard
            both_ref[at : at + shard, h * ports : (h + 1) * ports] = rows_ref[block, core]


def half_profit(both, returns_ref, t, half, start, count):
    paths, assets = returns_ref.shape[1:]
    columns = pl.ds(pl.multiple_of(half * (assets // 2), assets // 2), assets // 2)
    rows = [returns_ref[t, pl.ds(h * (paths // 2) + start, count), columns] for h in range(2)]
    return jnp.dot(jnp.concatenate(rows, axis=1), both, preferred_element_type=jnp.float32)


def first_kernel(shard, rows_ref, returns_ref, out_ref, both_ref):
    half = lax.axis_index("paths") // (lax.axis_size("paths") // 2)
    lay_out(shard, rows_ref, both_ref)
    both = both_ref[...]
    for t in range(returns_ref.shape[0]):
        out_ref[t] = half_profit(both, returns_ref, t, half, 0, out_ref.shape[1])


def scale_of(terms):
    return 2.0 ** math.floor(math.log2(65504 / (terms * MAX_RETURN * MAX_WEIGHT)))


def encode(part, terms):
    part = part * scale_of(terms)
    return jnp.where(part < SMALLEST, part * -FINER, part)


def decode(sent, terms):
    return jnp.where(sent < 0, sent * (-1 / (FINER * scale_of(terms))), sent * (1 / scale_of(terms)))


def second_kernel(segments, shard, tile, rows_ref, returns_ref, first_ref, *refs):
    out_ref, both_ref, stats = refs
    steps, paths, assets = returns_ref.shape
    ports = rows_ref.shape[1] // 2
    width = ports // segments
    half = 1 - lax.axis_index("paths") // (lax.axis_size("paths") // 2)
    lay_out(shard, rows_ref, both_ref)
    both = both_ref[...]
    stats[...] = jnp.zeros_like(stats)
    own = lax.axis_index("tm")
    block = min(128, paths // 2)
    for start in range(0, paths // 2, block):
        for g in range(0, steps, tile):
            profits = [
                half_profit(both, returns_ref, g + i, half, start, block) for i in range(tile)
            ]
            for q in range(0, block, 16):
                at = slice(start + q, start + q + 16)
                value, peak, low, fall = (stats[n, at] for n in range(4))
                for i in range(tile):
                    value = value + (first_ref[g + i, at] + profits[i][q : q + 16])
                    peak = jnp.maximum(peak, value)
                    low = jnp.minimum(low, value)
                    fall = jnp.maximum(fall, peak - value)
                for n, new in enumerate((value, peak, low, fall)):
                    stats[n, at] = new
        value, peak, low, fall = (stats[n, start : start + block] for n in range(4))
        for n, part in enumerate((fall, -low, peak - value, value - low)):
            turned = part.T
            for h in range(2):
                put = slice(h * (paths // 2) + start, h * (paths // 2) + start + block)
                for s in range(segments):
                    at = h * ports + s * width
                    exact = turned[at : at + width]
                    coded = encode(exact, steps * assets)
                    out_ref[own ^ s, n, :, put] = jnp.where(own == s, exact, coded)


def join_kernel(segments, terms, *refs):
    ins, out_ref, ordered = refs[:segments], refs[segments], refs[segments + 1]
    own = lax.axis_index("tm")
    for k in range(segments):
        ordered[own ^ k] = ins[0][0] if k == 0 else decode(ins[k][...], terms)
    fall = ordered[0, 0]
    drop = ordered[0, 2]
    for s in range(1, segments):
        below = ordered[s, 1]
        fall = jnp.maximum(jnp.maximum(fall, ordered[s, 0]), drop + below)
        drop = jnp.maximum(drop + below - ordered[s, 3], ordered[s, 2])
    out_ref[...] = fall


def shards(returns, weights):
    segments = lax.axis_size("tm")
    count = lax.axis_size("paths")
    steps, paths, assets = returns.shape
    shard, ports = weights.shape
    width = ports // segments
    held = jax.ShapeDtypeStruct((steps, paths // 2, 2 * ports), jnp.float32)
    both = pltpu.VMEM((assets, 2 * ports), weights.dtype)
    work = 2 * steps * paths * assets * ports

    rows = call(
        stage_kernel, "stage", jax.ShapeDtypeStruct(weights.shape, weights.dtype),
        [weights, returns], kept=(1,), flops=work, moved=returns.size * 2,
    )
    rows = call(
        pair_kernel, "pair", jax.ShapeDtypeStruct((shard, 2 * ports), rows.dtype),
        [rows, swap(weights, 1)],
    )
    bit = 2
    while 2 * bit < count:
        rows = call(
            functools.partial(merge_kernel, bit), f"merge{bit}",
            jax.ShapeDtypeStruct((2 * rows.shape[0], 2 * ports), rows.dtype),
            [rows, swap(rows, bit)],
        )
        bit *= 2
    other = swap(rows, bit)
    first = call(
        functools.partial(first_kernel, shard), "first", held, [rows, returns], scratch=[both],
        flops=work, moved=returns.size,
    )
    parts = call(
        functools.partial(second_kernel, segments, shard, min(steps, 8)), "second",
        jax.ShapeDtypeStruct((segments, 4, width, paths), jnp.float32), [other, returns, first],
        scratch=[both, pltpu.VMEM((4, paths // 2, 2 * ports), jnp.float32)],
        flops=work, moved=returns.size,
    )
    arrived = {
        k: lax.ppermute(
            parts[k].astype(jnp.float16), "tm", [(s, s ^ k) for s in range(segments)]
        ).astype(jnp.float32)
        for k in range(1, segments)
    }
    return call(
        functools.partial(join_kernel, segments, steps * assets), "join",
        jax.ShapeDtypeStruct((width, paths), jnp.float32),
        [parts] + [arrived[k] for k in range(1, segments)],
        scratch=[pltpu.VMEM((segments, 4, width, paths), jnp.float32)],
        moved=4 * parts.size,
    )


def solution(mesh):
    in_specs = (P("tm", "paths", None), P("paths", None))
    out_specs = P("tm", "paths")
    return jax.shard_map(shards, mesh=mesh, in_specs=in_specs, out_specs=out_specs, check_vma=False)
```

```python
import functools
import math

import jax
import jax.numpy as jnp
from jax import lax
from jax.experimental import pallas as pl
from jax.experimental.pallas import tpu as pltpu
from jax.sharding import PartitionSpec as P

SMALLEST = 2.0**-14
FINER = 2.0**28
MAX_RETURN = 0.15917969
MAX_WEIGHT = 0.375
VMEM = pl.BlockSpec(memory_space=pltpu.VMEM)
HBM = pl.BlockSpec(memory_space=pltpu.HBM)


def call(kernel, name, out_shape, args, scratch=(), kept=(), limit=8, flops=0, moved=0):
    args = [
        pltpu.with_memory_space_constraint(a, pltpu.HBM) if i in kept else a
        for i, a in enumerate(args)
    ]
    several = isinstance(out_shape, (list, tuple))
    return pl.pallas_call(
        kernel,
        out_shape=out_shape,
        in_specs=[HBM if i in kept else VMEM for i in range(len(args))],
        out_specs=[VMEM] * len(out_shape) if several else VMEM,
        scratch_shapes=list(scratch),
        compiler_params=pltpu.CompilerParams(vmem_limit_bytes=limit * 2**20),
        cost_estimate=pl.CostEstimate(flops=flops, bytes_accessed=moved, transcendentals=0),
        name=name,
    )(*args)


def swap(rows, bit):
    count = lax.axis_size("paths")
    return lax.ppermute(rows, "paths", [(s, s ^ (bit | 1)) for s in range(count)])


def stage_kernel(weights_ref, returns_ref, out_ref):
    out_ref[...] = weights_ref[...]


def pair_kernel(rows_ref, other_ref, out_ref):
    ports = rows_ref.shape[1]
    first = lax.axis_index("paths") % 2 == 0
    mine, other = rows_ref[...], other_ref[...]
    out_ref[:, :ports] = jnp.where(first, mine, other)
    out_ref[:, ports:] = jnp.where(first, other, mine)


def merge_kernel(bit, rows_ref, other_ref, out_ref):
    count = rows_ref.shape[0]
    upper = (lax.axis_index("paths") // bit) % 2
    out_ref[pl.ds(pl.multiple_of(upper * count, count), count)] = rows_ref[...]
    out_ref[pl.ds(pl.multiple_of((1 - upper) * count, count), count)] = other_ref[...]


def lay_out(shard, rows_ref, both_ref):
    ports = rows_ref.shape[1] // 2
    assets = both_ref.shape[0] // 2
    both_ref[...] = jnp.zeros_like(both_ref)
    for h in range(2):
        for n in range(assets // shard):
            block = slice(n // 2 * shard, (n // 2 + 1) * shard)
            core = slice(n % 2 * ports, (n % 2 + 1) * ports)
            at = h * assets + n * shard
            both_ref[at : at + shard, h * ports : (h + 1) * ports] = rows_ref[block, core]


def half_profit(both, returns_ref, t, half, start, count):
    paths, assets = returns_ref.shape[1:]
    columns = pl.ds(pl.multiple_of(half * (assets // 2), assets // 2), assets // 2)
    rows = [returns_ref[t, pl.ds(h * (paths // 2) + start, count), columns] for h in range(2)]
    return jnp.dot(jnp.concatenate(rows, axis=1), both, preferred_element_type=jnp.float32)


def first_kernel(shard, rows_ref, returns_ref, out_ref, both_ref):
    half = lax.axis_index("paths") // (lax.axis_size("paths") // 2)
    lay_out(shard, rows_ref, both_ref)
    both = both_ref[...]
    for t in range(returns_ref.shape[0]):
        out_ref[t] = half_profit(both, returns_ref, t, half, 0, out_ref.shape[1])


def scale_of(terms):
    return 2.0 ** math.floor(math.log2(65504 / (terms * MAX_RETURN * MAX_WEIGHT)))


def encode(part, terms):
    part = part * scale_of(terms)
    return jnp.where(part < SMALLEST, part * -FINER, part)


def decode(sent, terms):
    return jnp.where(sent < 0, sent * (-1 / (FINER * scale_of(terms))), sent * (1 / scale_of(terms)))


def second_kernel(segments, shard, tile, rows_ref, returns_ref, first_ref, *refs):
    out_ref, both_ref, stats = refs
    steps, paths, assets = returns_ref.shape
    ports = rows_ref.shape[1] // 2
    width = ports // segments
    half = 1 - lax.axis_index("paths") // (lax.axis_size("paths") // 2)
    lay_out(shard, rows_ref, both_ref)
    both = both_ref[...]
    stats[...] = jnp.zeros_like(stats)
    own = lax.axis_index("tm")
    block = min(128, paths // 2)
    for start in range(0, paths // 2, block):
        for g in range(0, steps, tile):
            profits = [
                half_profit(both, returns_ref, g + i, half, start, block) for i in range(tile)
            ]
            for q in range(0, block, 16):
                at = slice(start + q, start + q + 16)
                value, peak, low, fall = (stats[n, at] for n in range(4))
                for i in range(tile):
                    value = value + (first_ref[g + i, at] + profits[i][q : q + 16])
                    peak = jnp.maximum(peak, value)
                    low = jnp.minimum(low, value)
                    fall = jnp.maximum(fall, peak - value)
                for n, new in enumerate((value, peak, low, fall)):
                    stats[n, at] = new
        value, peak, low, fall = (stats[n, start : start + block] for n in range(4))
        for n, part in enumerate((fall, -low, peak - value, value - low)):
            turned = part.T
            for h in range(2):
                put = slice(h * (paths // 2) + start, h * (paths // 2) + start + block)
                for s in range(segments):
                    at = h * ports + s * width
                    exact = turned[at : at + width]
                    coded = encode(exact, steps * assets)
                    out_ref[own ^ s, n, :, put] = jnp.where(own == s, exact, coded)


def join_two(a, b):
    end = a[3] - a[1]
    below = jnp.maximum(a[1], b[1] - end)
    return (
        jnp.maximum(jnp.maximum(a[0], b[0]), a[2] + b[1]),
        below,
        jnp.maximum(a[2] + b[1] - b[3], b[2]),
        end + (b[3] - b[1]) + below,
    )


def join_tree(nodes, bit):
    own = lax.axis_index("tm")
    while len(nodes) > 1:
        later = (own // bit) % 2 == 1
        nodes = [
            join_two(
                [jnp.where(later, y, x) for x, y in zip(a, b)],
                [jnp.where(later, x, y) for x, y in zip(a, b)],
            )
            for a, b in zip(nodes[::2], nodes[1::2])
        ]
        bit *= 2
    return nodes[0]


def far_kernel(terms, *refs):
    nodes = [[decode(ref[n], terms) for n in range(4)] for ref in refs[:-1]]
    for n, part in enumerate(join_tree(nodes, 1)):
        refs[-1][n] = part


def join_kernel(terms, own_ref, *refs):
    near, (far_ref, out_ref) = refs[:-2], refs[-2:]
    nodes = [[own_ref[0, n] for n in range(4)]]
    nodes += [[decode(ref[n], terms) for n in range(4)] for ref in near]
    far = [far_ref[n] for n in range(4)]
    out_ref[...] = join_tree([join_tree(nodes, 1), far], len(nodes))[0]


def shards(returns, weights):
    segments = lax.axis_size("tm")
    count = lax.axis_size("paths")
    steps, paths, assets = returns.shape
    shard, ports = weights.shape
    width = ports // segments
    held = jax.ShapeDtypeStruct((steps, paths // 2, 2 * ports), jnp.float32)
    both = pltpu.VMEM((assets, 2 * ports), weights.dtype)
    work = 2 * steps * paths * assets * ports

    rows = call(
        stage_kernel, "stage", jax.ShapeDtypeStruct(weights.shape, weights.dtype),
        [weights, returns], kept=(1,), flops=work, moved=returns.size * 2,
    )
    rows = call(
        pair_kernel, "pair", jax.ShapeDtypeStruct((shard, 2 * ports), rows.dtype),
        [rows, swap(weights, 1)],
    )
    bit = 2
    while 2 * bit < count:
        rows = call(
            functools.partial(merge_kernel, bit), f"merge{bit}",
            jax.ShapeDtypeStruct((2 * rows.shape[0], 2 * ports), rows.dtype),
            [rows, swap(rows, bit)],
        )
        bit *= 2
    other = swap(rows, bit)
    first = call(
        functools.partial(first_kernel, shard), "first", held, [rows, returns], scratch=[both],
        flops=work, moved=returns.size,
    )
    parts = call(
        functools.partial(second_kernel, segments, shard, min(steps, 32)), "second",
        jax.ShapeDtypeStruct((segments, 4, width, paths), jnp.float32), [other, returns, first],
        scratch=[both, pltpu.VMEM((4, paths // 2, 2 * ports), jnp.float32)],
        flops=work, moved=returns.size,
    )
    arrived = {
        k: lax.ppermute(
            parts[k].astype(jnp.float16), "tm", [(s, s ^ k) for s in range(segments)]
        ).astype(jnp.float32)
        for k in range(1, segments)
    }
    far = call(
        functools.partial(far_kernel, steps * assets), "far",
        jax.ShapeDtypeStruct((4, width, paths), jnp.float32),
        [arrived[k] for k in range(segments // 2, segments)], moved=parts.size,
    )
    return call(
        functools.partial(join_kernel, steps * assets), "join",
        jax.ShapeDtypeStruct((width, paths), jnp.float32),
        [parts] + [arrived[k] for k in range(1, segments // 2)] + [far], moved=4 * parts.size,
    )


def solution(mesh):
    in_specs = (P("tm", "paths", None), P("paths", None))
    out_specs = P("tm", "paths")
    return jax.shard_map(shards, mesh=mesh, in_specs=in_specs, out_specs=out_specs, check_vma=False)
```

```python
import functools
import math

import jax
import jax.numpy as jnp
from jax import lax
from jax.experimental import pallas as pl
from jax.experimental.pallas import tpu as pltpu
from jax.sharding import PartitionSpec as P


SMALLEST = 2.0**-14
FINER = 2.0**28
MAX_RETURN = 0.15917969
MAX_WEIGHT = 0.375
VMEM = pl.BlockSpec(memory_space=pltpu.VMEM)
HBM = pl.BlockSpec(memory_space=pltpu.HBM)


def call(kernel, out_shape, args, scratch=(), kept=(), limit=8, flops=0, moved=0):
    args = [
        pltpu.with_memory_space_constraint(a, pltpu.HBM) if i in kept else a
        for i, a in enumerate(args)
    ]
    several = isinstance(out_shape, (list, tuple))
    return pl.pallas_call(
        kernel,
        out_shape=out_shape,
        in_specs=[HBM if i in kept else VMEM for i in range(len(args))],
        out_specs=[VMEM] * len(out_shape) if several else VMEM,
        scratch_shapes=list(scratch),
        compiler_params=pltpu.CompilerParams(vmem_limit_bytes=limit * 2**20),
        cost_estimate=pl.CostEstimate(flops=flops, bytes_accessed=moved, transcendentals=0),
    )(*args)


def swap(rows, bit):
    count = lax.axis_size("paths")
    return lax.ppermute(rows, "paths", [(s, s ^ (bit | 1)) for s in range(count)])


def stage_kernel(weights_ref, returns_ref, out_ref):
    out_ref[...] = weights_ref[...]


def pair_kernel(rows_ref, other_ref, out_ref):
    ports = rows_ref.shape[1]
    first = lax.axis_index("paths") % 2 == 0
    mine, other = rows_ref[...], other_ref[...]
    out_ref[:, :ports] = jnp.where(first, mine, other)
    out_ref[:, ports:] = jnp.where(first, other, mine)


def merge_kernel(bit, rows_ref, other_ref, out_ref):
    count = rows_ref.shape[0]
    upper = (lax.axis_index("paths") // bit) % 2
    out_ref[pl.ds(pl.multiple_of(upper * count, count), count)] = rows_ref[...]
    out_ref[pl.ds(pl.multiple_of((1 - upper) * count, count), count)] = other_ref[...]


def lay_out(shard, rows_ref, both_ref):
    ports = rows_ref.shape[1] // 2
    assets = both_ref.shape[0] // 2
    both_ref[...] = jnp.zeros_like(both_ref)
    for h in range(2):
        for n in range(assets // shard):
            block = slice(n // 2 * shard, (n // 2 + 1) * shard)
            core = slice(n % 2 * ports, (n % 2 + 1) * ports)
            at = h * assets + n * shard
            both_ref[at : at + shard, h * ports : (h + 1) * ports] = rows_ref[block, core]


def half_profit(both, returns_ref, t, half, start, count):
    paths, assets = returns_ref.shape[1:]
    columns = pl.ds(pl.multiple_of(half * (assets // 2), assets // 2), assets // 2)
    rows = [returns_ref[t, pl.ds(h * (paths // 2) + start, count), columns] for h in range(2)]
    return jnp.dot(jnp.concatenate(rows, axis=1), both, preferred_element_type=jnp.float32)


def first_kernel(shard, rows_ref, returns_ref, out_ref, both_ref):
    half = lax.axis_index("paths") // (lax.axis_size("paths") // 2)
    lay_out(shard, rows_ref, both_ref)
    both = both_ref[...]
    for t in range(returns_ref.shape[0]):
        out_ref[t] = half_profit(both, returns_ref, t, half, 0, out_ref.shape[1])


def scale_of(terms):
    return 2.0 ** math.floor(math.log2(65504 / (terms * MAX_RETURN * MAX_WEIGHT)))


def encode(part, terms):
    part = part * scale_of(terms)
    return jnp.where(part < SMALLEST, part * -FINER, part)


def decode(sent, terms):
    return jnp.where(sent < 0, sent * (-1 / (FINER * scale_of(terms))), sent * (1 / scale_of(terms)))


def second_kernel(segments, shard, tile, rows_ref, returns_ref, first_ref, *refs):
    out_ref, both_ref, stats = refs
    steps, paths, assets = returns_ref.shape
    ports = rows_ref.shape[1] // 2
    width = ports // segments
    half = 1 - lax.axis_index("paths") // (lax.axis_size("paths") // 2)
    lay_out(shard, rows_ref, both_ref)
    both = both_ref[...]
    stats[...] = jnp.zeros_like(stats)
    own = lax.axis_index("tm")
    block = min(128, paths // 2)
    for start in range(0, paths // 2, block):
        for g in range(0, steps, tile):
            profits = [
                half_profit(both, returns_ref, g + i, half, start, block) for i in range(tile)
            ]
            for q in range(0, block, 16):
                at = slice(start + q, start + q + 16)
                value, peak, low, fall = (stats[n, at] for n in range(4))
                for i in range(tile):
                    value = value + (first_ref[g + i, at] + profits[i][q : q + 16])
                    peak = jnp.maximum(peak, value)
                    low = jnp.minimum(low, value)
                    fall = jnp.maximum(fall, peak - value)
                for n, new in enumerate((value, peak, low, fall)):
                    stats[n, at] = new
        value, peak, low, fall = (stats[n, start : start + block] for n in range(4))
        for n, part in enumerate((fall, -low, peak - value, value - low)):
            turned = part.T
            for h in range(2):
                put = slice(h * (paths // 2) + start, h * (paths // 2) + start + block)
                for s in range(segments):
                    at = h * ports + s * width
                    exact = turned[at : at + width]
                    coded = encode(exact, steps * assets)
                    out_ref[own ^ s, n, :, put] = jnp.where(own == s, exact, coded)


def join_two(a, b):
    end = a[3] - a[1]
    below = jnp.maximum(a[1], b[1] - end)
    return (
        jnp.maximum(jnp.maximum(a[0], b[0]), a[2] + b[1]),
        below,
        jnp.maximum(a[2] + b[1] - b[3], b[2]),
        end + (b[3] - b[1]) + below,
    )


def join_tree(nodes, bit):
    own = lax.axis_index("tm")
    while len(nodes) > 1:
        later = (own // bit) % 2 == 1
        nodes = [
            join_two(
                [jnp.where(later, y, x) for x, y in zip(a, b)],
                [jnp.where(later, x, y) for x, y in zip(a, b)],
            )
            for a, b in zip(nodes[::2], nodes[1::2])
        ]
        bit *= 2
    return nodes[0]


def far_kernel(terms, *refs):
    nodes = [[decode(ref[n], terms) for n in range(4)] for ref in refs[:-1]]
    for n, part in enumerate(join_tree(nodes, 1)):
        refs[-1][n] = part


def join_kernel(terms, own_ref, *refs):
    near, (far_ref, out_ref) = refs[:-2], refs[-2:]
    nodes = [[own_ref[0, n] for n in range(4)]]
    nodes += [[decode(ref[n], terms) for n in range(4)] for ref in near]
    far = [far_ref[n] for n in range(4)]
    out_ref[...] = join_tree([join_tree(nodes, 1), far], len(nodes))[0]


def shards(returns, weights):
    segments = lax.axis_size("tm")
    count = lax.axis_size("paths")
    steps, paths, assets = returns.shape
    shard, ports = weights.shape
    width = ports // segments
    held = jax.ShapeDtypeStruct((steps, paths // 2, 2 * ports), jnp.float32)
    both = pltpu.VMEM((assets, 2 * ports), weights.dtype)
    work = 2 * steps * paths * assets * ports

    rows = call(
        stage_kernel, jax.ShapeDtypeStruct(weights.shape, weights.dtype),
        [weights, returns], kept=(1,), flops=work, moved=returns.size * 2,
    )
    rows = call(
        pair_kernel, jax.ShapeDtypeStruct((shard, 2 * ports), rows.dtype),
        [rows, swap(weights, 1)],
    )
    bit = 2
    while 2 * bit < count:
        rows = call(
            functools.partial(merge_kernel, bit),
            jax.ShapeDtypeStruct((2 * rows.shape[0], 2 * ports), rows.dtype),
            [rows, swap(rows, bit)],
        )
        bit *= 2
    other = swap(rows, bit)
    first = call(
        functools.partial(first_kernel, shard), held, [rows, returns], scratch=[both],
        flops=work, moved=returns.size,
    )
    parts = call(
        functools.partial(second_kernel, segments, shard, min(steps, 32)),
        jax.ShapeDtypeStruct((segments, 4, width, paths), jnp.float32), [other, returns, first],
        scratch=[both, pltpu.VMEM((4, paths // 2, 2 * ports), jnp.float32)],
        flops=work, moved=returns.size,
    )
    arrived = {}
    for k in range(1, segments):
        sent = lax.optimization_barrier(parts[k]).astype(jnp.float16)
        pairs = [(s, s ^ k) for s in range(segments)]
        arrived[k] = lax.ppermute(sent, "tm", pairs).astype(jnp.float32)
    far = call(
        functools.partial(far_kernel, steps * assets),
        jax.ShapeDtypeStruct((4, width, paths), jnp.float32),
        [arrived[k] for k in range(segments // 2, segments)], moved=parts.size,
    )
    return call(
        functools.partial(join_kernel, steps * assets),
        jax.ShapeDtypeStruct((width, paths), jnp.float32),
        [parts] + [arrived[k] for k in range(1, segments // 2)] + [far], moved=4 * parts.size,
    )


def solution(mesh):
    in_specs = (P("tm", "paths", None), P("paths", None))
    out_specs = P("tm", "paths")
    return jax.shard_map(
        shards, mesh=mesh, in_specs=in_specs, out_specs=out_specs, check_vma=False
    )
```
